32 devices in a mesh: row: 4 (over y, core), col: 8 (over z, x).
Axes of the slice: x: 2, y: 2, z: 4, core: 2. Of those that a mesh axis runs over, the one named last changes fastest.
Arguments:
- rhs: bfloat16 [6144, 6144], P('row', 'col'), may hold values from -6 to 6
- basis_left: bfloat16 [6144, 6144], P('col', 'row'), may hold values from -1 to 1, as said below
- basis_right: bfloat16 [6144, 6144], P('row', 'col'), may hold values from -1 to 1, as said below
- eig_left: float32 [6144], P('row'), may hold values from 0.1 to 4
- eig_right: float32 [6144], P('col'), may hold values from 0.1 to 4
Outputs:
- solution: bfloat16 [6144, 6144], P('col', 'row')
The draws below stay inside these ranges and needn't reach their ends.
Inputs may be any that keep to these rules, and one draw needn't show every extreme that they name: `basis_left`: an orthogonal matrix drawn uniformly, rounded to bfloat16. `basis_right`: an orthogonal matrix drawn uniformly, rounded to bfloat16.
All inputs are finite; a program needn't handle non-finite values.
Results may differ from the reference program's by a relative error of at most 0.0085.
Values may be sent and summed in bfloat16 or wider, within the bound.
A program may use at most 128 MiB of HBM per device.

```python
import math
import jax
import jax.numpy as jnp

N = 6144


def orthogonal_matrix(key):
    normal_draw = jax.random.normal(key, (N, N), jnp.float32)
    factor_q, factor_r = jnp.linalg.qr(normal_draw)
    signs = jnp.where(jnp.diagonal(factor_r) < 0.0, -1.0, 1.0).astype(jnp.float32)
    return (factor_q * signs[None, :]).astype(jnp.bfloat16)


def draw_basis_left(key, part):
    return orthogonal_matrix(jax.random.fold_in(key, 11))


def draw_basis_right(key, part):
    return orthogonal_matrix(jax.random.fold_in(key, 23))


def block_levels(key, shape, pieces, smallest, top_value):
    level = 1.0
    for dim, parts in pieces:
        steps = jax.random.uniform(jax.random.fold_in(jax.random.fold_in(key, 6), dim), (parts,), jnp.float32, smallest / len(pieces), top_value / len(pieces))
        level = level * jnp.repeat(jnp.exp(steps), shape[dim] // parts).reshape((-1,) + (1,) * (len(shape) - 1 - dim))
    return level


def normal_values(own_key, extent, width, reach, cuts=(), kind=jnp.bfloat16):
    loudness = block_levels(own_key, extent, cuts, -0.22, 0.18) if cuts else 1.0
    array = jax.random.normal(own_key, extent, jnp.float32) * width * loudness
    return jnp.minimum(jnp.maximum(array, -reach), reach).astype(kind)


def setup_inputs(seed: int = 0) -> dict:
    key_list = jax.random.split(jax.random.key(seed), 6)
    return {
        "rhs": normal_values(key_list[0], (N, N), 1.0, 6.0, ((0, 4), (1, 8))),
        "basis_left": draw_basis_left(jax.random.fold_in(key_list[5], 71), 0),
        "basis_right": draw_basis_right(jax.random.fold_in(key_list[5], 71), 0),
        "eig_left": jnp.clip(jnp.exp(math.log(4.0) - 3.6888794 * jax.random.uniform(key_list[3], (N,), jnp.float32) ** block_levels(key_list[3], (N,), ((0, 4),), -0.2, 0.2)), 0.1, 4.0),
        "eig_right": jnp.clip(jnp.exp(math.log(4.0) - 3.6888794 * jax.random.uniform(key_list[4], (N,), jnp.float32) ** block_levels(key_list[4], (N,), ((0, 8),), -0.2, 0.2)), 0.1, 4.0),
    }


def reference(rhs, basis_left, basis_right, eig_left, eig_right):
    projected = jnp.dot(basis_left.T.astype(jnp.float32), rhs.astype(jnp.float32), preferred_element_type=jnp.float32).astype(jnp.bfloat16)
    second = jnp.dot(projected.astype(jnp.float32), basis_right.astype(jnp.float32), preferred_element_type=jnp.float32)
    scaled = (second / (eig_left[:, None] + eig_right[None, :])).astype(jnp.bfloat16)
    half = jnp.dot(basis_left.astype(jnp.float32), scaled.astype(jnp.float32), preferred_element_type=jnp.float32).astype(jnp.bfloat16)
    return jnp.dot(half.astype(jnp.float32), basis_right.T.astype(jnp.float32), preferred_element_type=jnp.float32).astype(jnp.bfloat16)
```

```python
import functools
import jax
import jax.numpy as jnp
from jax import lax
from jax.experimental import pallas as pl
from jax.experimental.pallas import tpu as pltpu
from jax.sharding import PartitionSpec as P

BF16, F32 = jnp.bfloat16, jnp.float32

NC = 2
NL = 2
I_CHUNKS = 3
R_CHUNKS = 3


def hop(a, axis, mask):
    n = lax.axis_size(axis)
    return lax.ppermute(a, axis, [(i, i ^ mask) for i in range(n)])


def ordered(pieces, me):
    bit = 1
    while bit < len(pieces):
        odd = (me & bit) != 0
        pieces = [jnp.where(odd, pieces[p ^ bit], pieces[p]) for p in range(len(pieces))]
        bit *= 2
    return pieces


def gather(a, axis, unit, g, me):
    return ordered([a] + [hop(a, axis, unit * s) for s in range(1, g)], me)


def part(a, i, n, dim=0):
    return lax.dynamic_slice_in_dim(a, i * n, n, axis=dim)


def body(nz, nx, rhs, basis_left, basis_right, eig_left, eig_right):
    col, row = lax.axis_index("col"), lax.axis_index("row")
    ny, nh = lax.axis_size("row") // NC, nz // NL
    x, z = lax.rem(col, nx), lax.div(col, nx)
    zl, zh = lax.rem(z, NL), lax.div(z, NL)
    c, y = lax.rem(row, NC), lax.div(row, NC)
    ZL, ZH = nx, nx * NL

    def panel(a):
        cols = []
        for b in [a, hop(a, "col", ZL)]:
            over_y = [b] + [hop(b, "row", NC * s) for s in range(1, ny)]
            over_c = [hop(b, "row", 1) for b in over_y]
            quarters = []
            for u, v in zip(over_y, over_c):
                quarters += [u, v]
            cols.append(ordered(quarters, row))
        both = ordered([jnp.concatenate(q, axis=0) for q in cols], zl)
        return jnp.concatenate(both, axis=1)

    rows_own, cols_own = basis_left.shape
    width = cols_own // NL
    w = width // I_CHUNKS

    def left_chunk(m):
        mine = lax.dynamic_slice_in_dim(basis_left, zl * width + m * w, w, axis=1)
        theirs = lax.dynamic_slice_in_dim(basis_left, (zl ^ 1) * width + m * w, w, axis=1)
        a = ordered([mine, hop(theirs, "col", ZL)], zl)
        a = jnp.stack(a)
        a = jnp.stack(gather(a, "col", ZH, nh, zh))
        a = jnp.stack(gather(a, "col", 1, nx, x), axis=2)
        return a.reshape(nh * NL * nx * rows_own, w)

    left = [left_chunk(m) for m in range(I_CHUNKS)]
    c_panel = panel(rhs)
    b_panel = panel(basis_right)
    er = jnp.concatenate(gather(eig_right, "col", ZL, NL, zl))
    el = lax.dynamic_slice_in_dim(eig_left, zl * width, width, axis=0)

    scaled = []
    for m in range(I_CHUNKS):
        p = lax.dot_general(left[m], c_panel, (((0,), (0,)), ((), ())), preferred_element_type=F32).astype(BF16)
        p = p.reshape(w, NL, -1)
        p = jnp.stack(gather(p, "col", ZH, nh, zh), axis=1)
        p = jnp.stack(gather(p, "col", 1, nx, x), axis=3)
        p = p.reshape(w, -1)
        second = jnp.dot(p, b_panel, preferred_element_type=F32)
        scaled.append((second / (el[m * w:(m + 1) * w, None] + er[None, :])).astype(BF16))
    scaled = jnp.concatenate(scaled, axis=0)

    sub = rows_own // (ny * NC * R_CHUNKS)
    qa = jnp.concatenate(left, axis=1)
    qa = qa.reshape(nh, NL, nx, ny, NC, R_CHUNKS, sub, width)
    qa = qa.transpose(5, 4, 3, 1, 2, 0, 6, 7).reshape(R_CHUNKS, -1, width)
    rows = qa.shape[1]

    def add_hops(total, parts, axis, unit):
        for s in range(1, len(parts) + 1):
            total = total + hop(parts[s - 1].astype(BF16), axis, unit * s).astype(F32)
        return total

    def scatter(v, axis, unit, g, me):
        n = v.shape[0] // g
        return add_hops(part(v, me, n), [part(v, me ^ s, n) for s in range(1, g)], axis, unit)

    outs = []
    for q in range(R_CHUNKS):
        half_rows = rows // NC
        give = jnp.dot(part(qa[q], c ^ 1, half_rows), scaled, preferred_element_type=F32)
        keep = jnp.dot(part(qa[q], c, half_rows), scaled, preferred_element_type=F32)
        h = add_hops(keep, [give], "row", 1)
        h = scatter(h, "row", NC, ny, y)
        h = scatter(h, "col", ZL, NL, zl).astype(BF16)
        n = h.shape[0] // nx

        def term(i):
            return lax.dot_general(part(h, i, n), b_panel, (((1,), (1,)), ((), ())), preferred_element_type=F32)

        give = [term(x ^ s) for s in range(1, nx)]
        t = add_hops(term(x), give, "col", 1)
        t = scatter(t, "col", ZH, nh, zh).astype(BF16)
        t = t.reshape(sub, ny * NC, -1)
        got = [lax.dynamic_index_in_dim(t, row, 1, keepdims=False)]
        for s in range(1, ny * NC):
            got.append(hop(lax.dynamic_index_in_dim(t, row ^ s, 1, keepdims=False), "row", s))
        outs.append(jnp.stack(ordered(got, row)))
    return jnp.stack(outs, axis=1).reshape(rows_own, cols_own)


MESH = pl.DeviceIdType.MESH
W = 256
PIECES = 3
NR = 6
VMEM_LIMIT = 67043328


def place():
    col, row = lax.axis_index("col"), lax.axis_index("row")
    x, z = col % 2, col // 2
    return row // 2, row % 2, z // 2, z % 2, x


def device(y, c, zh, zl, x):
    return (y * 2 + c, (zh * 2 + zl) * 2 + x)


def enter(partners):
    barrier = pltpu.get_barrier_semaphore()
    for d in partners:
        pl.semaphore_signal(barrier, inc=1, device_id=d, device_id_type=MESH)
    pl.semaphore_wait(barrier, len(partners))


def first_kernel(rhs, ql, qr, el, er, s_out, qa_out, b_out,
                 cp, bp, qa, qat, pbuf, s, erb, send, recv, local):
    y, c, zh, zl, x = place()
    ry, rc = device(1 - y, c, zh, zl, x), device(y, 1 - c, zh, zl, x)
    rl, rh, rx = device(y, c, zh, 1 - zl, x), device(y, c, 1 - zh, zl, x), device(y, c, zh, zl, 1 - x)
    enter([ry, rc, rl, rh, rx])
    r0, c0 = rhs.shape
    chunks = c0 // W
    rp = r0 // PIECES
    ids = {}

    def push(key, src, dst, dev):
        k = ids.setdefault(key, len(ids))
        d = pltpu.make_async_remote_copy(src_ref=src, dst_ref=dst, send_sem=send.at[k], recv_sem=recv.at[k],
                                         device_id=dev, device_id_type=MESH)
        d.start()
        started[key] = d

    started = {}

    def got(key):
        started[key].wait_recv()

    def lanes(i):
        return pl.ds(pl.multiple_of(i, 128), W)

    def qa_at(m, a, b, d):
        return qa.at[m, a, b, d]

    def rows(yy, cc, p):
        return pl.ds(pl.multiple_of((yy * 2 + cc) * r0 + p * rp, 16), rp)

    own = [pltpu.make_async_copy(ql.at[:, :, :, lanes(zl * c0 + m * W)], qa_at(m, zh, zl, x), local.at[m]) for m in range(chunks)]
    own_c = pltpu.make_async_copy(rhs, cp.at[zl, pl.ds(pl.multiple_of((y * 2 + c) * r0, 16), r0)], local.at[chunks])
    own_b = pltpu.make_async_copy(qr, bp.at[zl, pl.ds(pl.multiple_of((y * 2 + c) * r0, 16), r0)], local.at[chunks + 1])
    own_e = pltpu.make_async_copy(er, erb.at[zl], local.at[chunks + 2])
    for d in own + [own_c, own_b, own_e]:
        d.start()

    def panel_push(t, ref, hopname, zz, yy, cc, p, dev):
        v = ref.at[zz, rows(yy, cc, p)]
        push((t, hopname, p), v, v, dev)

    def qa_own(m):
        push(("a", "l", m), ql.at[:, :, :, lanes((1 - zl) * c0 + m * W)], qa_at(m, zh, zl, x), rl)
        push(("a", "h0", m), qa_at(m, zh, zl, x), qa_at(m, zh, zl, x), rh)
        push(("a", "x00", m), qa_at(m, zh, zl, x), qa_at(m, zh, zl, x), rx)

    def qa_l(m):
        got(("a", "l", m))
        v = qa_at(m, zh, 1 - zl, x)
        push(("a", "h1", m), v, v, rh)
        push(("a", "x01", m), v, v, rx)

    def qa_h0(m):
        got(("a", "h0", m))
        v = qa_at(m, 1 - zh, zl, x)
        push(("a", "x10", m), v, v, rx)

    def qa_h1(m):
        got(("a", "h1", m))
        v = qa_at(m, 1 - zh, 1 - zl, x)
        push(("a", "x11", m), v, v, rx)

    def panel_l(t, ref, p):
        got((t, "l", p))
        panel_push(t, ref, "y1", 1 - zl, y, c, p, ry)
        panel_push(t, ref, "c10", 1 - zl, y, c, p, rc)

    def panel_y0(t, ref, p):
        got((t, "y0", p))
        panel_push(t, ref, "c01", zl, 1 - y, c, p, rc)

    def panel_y1(t, ref, p):
        got((t, "y1", p))
        panel_push(t, ref, "c11", 1 - zl, 1 - y, c, p, rc)

    for d in own:
        d.wait()
    own_c.wait()
    qa_own(0)
    for p in range(PIECES):
        panel_push("c", cp, "l", zl, y, c, p, rl)
        panel_push("c", cp, "y0", zl, y, c, p, ry)
        panel_push("c", cp, "c00", zl, y, c, p, rc)
        if p + 1 < chunks:
            qa_own(p + 1)
    for m in range(PIECES + 1, chunks):
        qa_own(m)
    own_e.wait()
    push(("e",), erb.at[zl], erb.at[zl], rl)
    own_b.wait()
    for p in range(PIECES):
        panel_push("b", bp, "c00", zl, y, c, p, rc)

    for m in range(chunks):
        qa_l(m)
        if m < PIECES:
            panel_l("c", cp, m)
        qa_h0(m)
        if m < PIECES:
            panel_y0("c", cp, m)
        if m >= 1:
            qa_h1(m - 1)
            if m - 1 < PIECES:
                panel_y1("c", cp, m - 1)
    for p in range(PIECES):
        panel_push("b", bp, "l", zl, y, c, p, rl)
        panel_push("b", bp, "y0", zl, y, c, p, ry)
    qa_h1(chunks - 1)
    for p in range(chunks, PIECES):
        panel_l("c", cp, p)
        panel_y0("c", cp, p)
    for p in range(chunks - 1, PIECES):
        panel_y1("c", cp, p)
    for h in ("c00", "c10", "c01", "c11"):
        for p in range(PIECES):
            got(("c", h, p))

    tiles = 2 * c0 // W
    per = c0 // W

    def project(m):
        for h in ("x00", "x01", "x10", "x11"):
            got(("a", h, m))
        for a in range(2):
            for b in range(2):
                for d in range(2):
                    k = ((a * 2 + b) * 2 + d) * c0
                    qat[:, k:k + c0] = qa[m, a, b, d].reshape(c0, W).T

        @pl.loop(0, tiles)
        def _(nt):
            acc = jnp.dot(qat[...], cp[nt // per, :, pl.ds(pl.multiple_of(nt % per * W, W), W)], preferred_element_type=F32)
            pbuf[m, zh, x, :, pl.ds(pl.multiple_of(nt * W, W), W)] = acc.astype(BF16)

        v = pbuf.at[m, zh, x]
        push(("p", "h", m), v, v, rh)
        push(("p", "x0", m), v, v, rx)

    def forward(m):
        got(("p", "h", m))
        v = pbuf.at[m, 1 - zh, x]
        push(("p", "x1", m), v, v, rx)

    def second(m):
        got(("p", "x0", m))
        got(("p", "x1", m))

        @pl.loop(0, tiles)
        def _(nt):
            acc = None
            for a in range(2):
                for d in range(2):
                    for b in range(2):
                        k = ((a * 2 + b) * 2 + d) * c0
                        t = jnp.dot(pbuf[m, a, d, :, b * c0:(b + 1) * c0],
                                    bp[nt // per, k:k + c0, pl.ds(pl.multiple_of(nt % per * W, W), W)],
                                    preferred_element_type=F32)
                        acc = t if acc is None else acc + t
            den = el[m * W:(m + 1) * W, :] + erb[nt // per, :, pl.ds(pl.multiple_of(nt % per * W, W), W)]
            s[m * W:(m + 1) * W, pl.ds(pl.multiple_of(nt * W, W), W)] = (acc / den).astype(BF16)

    for m in range(chunks):
        project(m)
        if m < PIECES:
            panel_l("b", bp, m)
            panel_y0("b", bp, m)
    for p in range(chunks, PIECES):
        panel_l("b", bp, p)
        panel_y0("b", bp, p)
    qa_copy = pltpu.make_async_copy(qa, qa_out, local.at[0])
    qa_copy.start()
    for m in range(chunks):
        forward(m)
        if m < PIECES:
            panel_y1("b", bp, m)
    for p in range(chunks, PIECES):
        panel_y1("b", bp, p)
    for h in ("c00", "c10", "c01", "c11"):
        for p in range(PIECES):
            got(("b", h, p))
    b_copy = pltpu.make_async_copy(bp, b_out, local.at[1])
    b_copy.start()
    got(("e",))
    for m in range(chunks):
        second(m)
    s_copy = pltpu.make_async_copy(s, s_out, local.at[2])
    s_copy.start()
    for d in started.values():
        d.wait_send()
    qa_copy.wait()
    b_copy.wait()
    s_copy.wait()


def second_kernel(qa_in, s_in, b_in, out, qa, s, b, recvc, recvy, recvl, givec, givey, givel, hf,
                  recvx, recvh, givex, giveh, fin, keep, send, recv, outs, outr, local):
    y, c, zh, zl, x = place()
    ry, rc = device(1 - y, c, zh, zl, x), device(y, 1 - c, zh, zl, x)
    rl, rh, rx = device(y, c, zh, 1 - zl, x), device(y, c, 1 - zh, zl, x), device(y, c, zh, zl, 1 - x)
    rd = device(1 - y, 1 - c, zh, zl, x)
    loads = [pltpu.make_async_copy(u, v, local.at[i]) for i, (u, v) in enumerate(((s_in, s), (qa_in, qa), (b_in, b)))]
    for d in loads:
        d.start()
    enter([ry, rc, rl, rh, rx, rd])
    chunks, c0 = qa.shape[0], b.shape[2]
    tiles = 2 * c0 // W
    quarter = out.shape[-1]
    T = 512
    per = quarter // T

    def hop_of(k, q, src, dst, dev):
        return pltpu.make_async_remote_copy(src_ref=src, dst_ref=dst, send_sem=send.at[k, q], recv_sem=recv.at[k, q],
                                            device_id=dev, device_id_type=MESH)

    def c_hop(q):
        return hop_of(0, q, givec, recvc.at[q], rc)

    def y_hop(q):
        return hop_of(1, q, givey.at[q % 2], recvy.at[q], ry)

    def l_hop(q):
        return hop_of(2, q, givel.at[q % 2], recvl.at[q], rl)

    def x_hop(q):
        return hop_of(3, q, givex.at[q % 2], recvx.at[q], rx)

    def h_hop(q):
        return hop_of(4, q, giveh.at[q % 2], recvh.at[q], rh)

    def out_hops(q):
        yc = y * 2 + c
        hops = []
        for i, (dev, to) in enumerate(((rc, y * 2 + 1 - c), (ry, (1 - y) * 2 + c), (rd, (1 - y) * 2 + 1 - c))):
            hops.append(pltpu.make_async_remote_copy(
                src_ref=fin.at[q % 2, to], dst_ref=out.at[yc, q], send_sem=outs.at[i, q], recv_sem=outr.at[i, q],
                device_id=dev, device_id_type=MESH))
        return hops

    def own_out(q):
        yc = y * 2 + c
        return pltpu.make_async_copy(fin.at[q % 2, yc], out.at[yc, q], local.at[3 + q % 2])

    def cols(nt, n):
        return pl.ds(pl.multiple_of(nt * n, n), n)

    def left_dot(load, nt):
        acc = None
        for m in range(chunks):
            a = load(m)
            a = a.reshape(-1, a.shape[-1])
            t = jnp.dot(a, s[m * W:(m + 1) * W, cols(nt, W)], preferred_element_type=F32)
            acc = t if acc is None else acc + t
        return acc

    def wide(v):
        return v.reshape(-1, v.shape[-1]).astype(F32)

    def stage_c(q):
        @pl.when(q >= 1)
        def _():
            c_hop(q - 1).wait_send()

        @pl.loop(0, 2 * tiles)
        def _(t):
            yy, nt = t // tiles, t % tiles
            acc = left_dot(lambda m: qa[m, :, :, :, yy * 2 + 1 - c, q], nt)
            givec[yy, :, :, :, :, cols(nt, W)] = acc.astype(BF16).reshape(givec.shape[1:5] + (W,))

        c_hop(q).start()

    def stage_y(q):
        c_hop(q).wait_recv()

        @pl.when(q >= 2)
        def _():
            y_hop(q - 2).wait_send()

        @pl.loop(0, tiles)
        def _(nt):
            acc = left_dot(lambda m: qa[m, :, :, :, (1 - y) * 2 + c, q], nt)
            acc = acc + wide(recvc[q, 1 - y, :, :, :, :, cols(nt, W)])
            givey[q % 2, :, :, :, :, cols(nt, W)] = acc.astype(BF16).reshape(givey.shape[1:5] + (W,))

        y_hop(q).start()

    def stage_l(q):
        y_hop(q).wait_recv()

        @pl.when(q >= 2)
        def _():
            l_hop(q - 2).wait_send()

        @pl.loop(0, tiles)
        def _(nt):
            acc = left_dot(lambda m: qa[m, :, 1 - zl, :, y * 2 + c, q], nt)
            acc = acc + wide(recvc[q, y, :, 1 - zl, :, :, cols(nt, W)]) + wide(recvy[q, :, 1 - zl, :, :, cols(nt, W)])
            givel[q % 2, :, :, :, cols(nt, W)] = acc.astype(BF16).reshape(givel.shape[1:4] + (W,))

        l_hop(q).start()

    def right_dot(h, ct):
        acc = None
        for k in range(2):
            t = lax.dot_general(h[:, k * c0:(k + 1) * c0], b[k, cols(ct, T), :], (((1,), (1,)), ((), ())), preferred_element_type=F32)
            acc = t if acc is None else acc + t
        return acc

    def stage_x(q):
        l_hop(q).wait_recv()

        @pl.loop(0, tiles)
        def _(nt):
            acc = left_dot(lambda m: qa[m, :, zl, :, y * 2 + c, q], nt)
            acc = acc + wide(recvc[q, y, :, zl, :, :, cols(nt, W)]) + wide(recvy[q, :, zl, :, :, cols(nt, W)])
            acc = acc + wide(recvl[q, :, :, :, cols(nt, W)])
            hf[q % 2, :, :, :, cols(nt, W)] = acc.astype(BF16).reshape(hf.shape[1:4] + (W,))

        @pl.when(q >= 2)
        def _():
            x_hop(q - 2).wait_send()

        @pl.when(q == 0)
        def _():
            loads[2].wait()

        @pl.loop(0, 4 * per)
        def _(ct):
            h = hf[q % 2, :, 1 - x].reshape(-1, 2 * c0)
            v = right_dot(h, ct).astype(BF16)
            givex[q % 2, :, ct // per, :, cols(ct % per, T)] = v.reshape(2, -1, T)

        x_hop(q).start()

    def stage_h(q):
        x_hop(q).wait_recv()

        @pl.when(q >= 2)
        def _():
            h_hop(q - 2).wait_send()

        @pl.loop(0, 4 * per)
        def _(ct):
            h = hf[q % 2, :, x].reshape(-1, 2 * c0)
            v = right_dot(h, ct) + wide(recvx[q, :, ct // per, :, cols(ct % per, T)])
            v = v.reshape(2, -1, T)
            low = zh == 0
            giveh[q % 2, ct // per, :, cols(ct % per, T)] = jnp.where(low, v[1], v[0]).astype(BF16)
            keep[q % 2, ct // per, :, cols(ct % per, T)] = jnp.where(low, v[0], v[1])

        h_hop(q).start()

    def stage_o(q):
        h_hop(q).wait_recv()

        @pl.when(q >= 2)
        def _():
            for d in out_hops(q - 2):
                d.wait_send()
            own_out(q - 2).wait()

        @pl.loop(0, 4)
        def _(i):
            fin[q % 2, i] = (keep[q % 2, i] + recvh[q, i].astype(F32)).astype(BF16)

        for d in out_hops(q):
            d.start()
        own_out(q).start()

    loads[0].wait()
    loads[1].wait()
    stages = (stage_c, stage_y, stage_l, stage_x, stage_h, stage_o)

    @pl.loop(0, NR + len(stages) - 1)
    def _(t):
        for lag, stage in enumerate(stages):
            @pl.when((t >= lag) & (t < lag + NR))
            def _(stage=stage, lag=lag):
                stage(t - lag)

    c_hop(NR - 1).wait_send()
    for q in (NR - 2, NR - 1):
        y_hop(q).wait_send()
        l_hop(q).wait_send()
        x_hop(q).wait_send()
        h_hop(q).wait_send()
        for d in out_hops(q):
            d.wait_send()
        own_out(q).wait()
    for q in range(NR):
        for d in out_hops(q):
            d.wait_recv()


def kernels(rhs, basis_left, basis_right, eig_left, eig_right):
    r0, c0 = rhs.shape
    n = 4 * r0
    chunks = c0 // W
    sub = c0 // (4 * NR)
    zl = lax.rem(lax.div(lax.axis_index("col"), 2), 2)
    el = lax.dynamic_slice_in_dim(eig_left, zl * c0, c0, axis=0)[:, None]
    any_spec = pl.BlockSpec(memory_space=pl.ANY)
    vmem = pl.BlockSpec(memory_space=pltpu.VMEM)
    qa_shape = (chunks, 2, 2, 2, 4, NR, sub, W)
    copies = 2 * 7 * PIECES + 10 * chunks + 1
    dma = pltpu.SemaphoreType.DMA
    s, qa, b = pl.pallas_call(
        first_kernel,
        out_shape=(jax.ShapeDtypeStruct((c0, 2 * c0), BF16), jax.ShapeDtypeStruct(qa_shape, BF16),
                   jax.ShapeDtypeStruct((2, n, c0), BF16)),
        in_specs=[any_spec, any_spec, any_spec, vmem, any_spec],
        out_specs=(any_spec, any_spec, any_spec),
        scratch_shapes=[
            pltpu.VMEM((2, n, c0), BF16), pltpu.VMEM((2, n, c0), BF16), pltpu.VMEM(qa_shape, BF16),
            pltpu.VMEM((W, n), BF16), pltpu.VMEM((chunks, 2, 2, W, 2 * c0), BF16), pltpu.VMEM((c0, 2 * c0), BF16),
            pltpu.VMEM((2, 1, c0), F32), dma((copies,)), dma((copies,)), dma((chunks + 3,))],
        compiler_params=pltpu.CompilerParams(collective_id=0, has_side_effects=True, vmem_limit_bytes=VMEM_LIMIT),
        name="first_half",
    )(rhs, basis_left.reshape(4, NR, sub, 2 * c0), basis_right, el, eig_right[None, :])
    out = pl.pallas_call(
        second_kernel,
        out_shape=jax.ShapeDtypeStruct((4, NR, sub, r0), BF16),
        in_specs=[any_spec] * 3,
        out_specs=any_spec,
        scratch_shapes=[
            pltpu.VMEM(qa_shape, BF16), pltpu.VMEM((c0, 2 * c0), BF16), pltpu.VMEM((2, n, c0), BF16),
            pltpu.VMEM((NR, 2, 2, 2, 2, sub, 2 * c0), BF16), pltpu.VMEM((NR, 2, 2, 2, sub, 2 * c0), BF16),
            pltpu.VMEM((NR, 2, 2, sub, 2 * c0), BF16),
            pltpu.VMEM((2, 2, 2, 2, sub, 2 * c0), BF16), pltpu.VMEM((2, 2, 2, 2, sub, 2 * c0), BF16),
            pltpu.VMEM((2, 2, 2, sub, 2 * c0), BF16), pltpu.VMEM((2, 2, 2, sub, 2 * c0), BF16),
            pltpu.VMEM((NR, 2, 4, sub, r0), BF16), pltpu.VMEM((NR, 4, sub, r0), BF16),
            pltpu.VMEM((2, 2, 4, sub, r0), BF16), pltpu.VMEM((2, 4, sub, r0), BF16),
            pltpu.VMEM((2, 4, sub, r0), BF16), pltpu.VMEM((2, 4, sub, r0), F32),
            dma((5, NR)), dma((5, NR)), dma((3, NR)), dma((3, NR)), dma((5,))],
        compiler_params=pltpu.CompilerParams(collective_id=1, has_side_effects=True, vmem_limit_bytes=VMEM_LIMIT),
        name="second_half",
    )(qa, s, b)
    return out.reshape(c0, r0)


def fits(nz, nx, ny, rows, cols):
    return nz == 4 and nx == 2 and ny == 2 and rows == 2 * cols and cols % (4 * NR * 16) == 0 and cols % W == 0 and rows % 512 == 0


def step(nz, nx, *arrays):
    rows, cols = arrays[0].shape
    if fits(nz, nx, lax.axis_size("row") // NC, rows, cols):
        return kernels(*arrays)
    return body(nz, nx, *arrays)


def solution(mesh):
    nz = mesh.shape["row"]
    nx = mesh.shape["col"] // nz
    in_specs = (P("row", "col"), P("col", "row"), P("row", "col"), P("row"), P("col"))
    fn = functools.partial(step, nz, nx)
    return jax.shard_map(fn, mesh=mesh, in_specs=in_specs, out_specs=P("col", "row"), check_vma=False)
```

```python
import functools
import jax
import jax.numpy as jnp
from jax import lax
from jax.experimental import pallas as pl
from jax.experimental.pallas import tpu as pltpu
from jax.sharding import PartitionSpec as P

BF16, F32 = jnp.bfloat16, jnp.float32

NC = 2
NL = 2
I_CHUNKS = 3
R_CHUNKS = 3


def hop(a, axis, mask):
    n = lax.axis_size(axis)
    return lax.ppermute(a, axis, [(i, i ^ mask) for i in range(n)])


def ordered(pieces, me):
    bit = 1
    while bit < len(pieces):
        odd = (me & bit) != 0
        pieces = [jnp.where(odd, pieces[p ^ bit], pieces[p]) for p in range(len(pieces))]
        bit *= 2
    return pieces


def gather(a, axis, unit, g, me):
    return ordered([a] + [hop(a, axis, unit * s) for s in range(1, g)], me)


def part(a, i, n, dim=0):
    return lax.dynamic_slice_in_dim(a, i * n, n, axis=dim)


def body(nz, nx, rhs, basis_left, basis_right, eig_left, eig_right):
    col, row = lax.axis_index("col"), lax.axis_index("row")
    ny, nh = lax.axis_size("row") // NC, nz // NL
    x, z = lax.rem(col, nx), lax.div(col, nx)
    zl, zh = lax.rem(z, NL), lax.div(z, NL)
    c, y = lax.rem(row, NC), lax.div(row, NC)
    ZL, ZH = nx, nx * NL

    def panel(a):
        cols = []
        for b in [a, hop(a, "col", ZL)]:
            over_y = [b] + [hop(b, "row", NC * s) for s in range(1, ny)]
            over_c = [hop(b, "row", 1) for b in over_y]
            quarters = []
            for u, v in zip(over_y, over_c):
                quarters += [u, v]
            cols.append(ordered(quarters, row))
        both = ordered([jnp.concatenate(q, axis=0) for q in cols], zl)
        return jnp.concatenate(both, axis=1)

    rows_own, cols_own = basis_left.shape
    width = cols_own // NL
    w = width // I_CHUNKS

    def left_chunk(m):
        mine = lax.dynamic_slice_in_dim(basis_left, zl * width + m * w, w, axis=1)
        theirs = lax.dynamic_slice_in_dim(basis_left, (zl ^ 1) * width + m * w, w, axis=1)
        a = ordered([mine, hop(theirs, "col", ZL)], zl)
        a = jnp.stack(a)
        a = jnp.stack(gather(a, "col", ZH, nh, zh))
        a = jnp.stack(gather(a, "col", 1, nx, x), axis=2)
        return a.reshape(nh * NL * nx * rows_own, w)

    left = [left_chunk(m) for m in range(I_CHUNKS)]
    c_panel = panel(rhs)
    b_panel = panel(basis_right)
    er = jnp.concatenate(gather(eig_right, "col", ZL, NL, zl))
    el = lax.dynamic_slice_in_dim(eig_left, zl * width, width, axis=0)

    scaled = []
    for m in range(I_CHUNKS):
        p = lax.dot_general(left[m], c_panel, (((0,), (0,)), ((), ())), preferred_element_type=F32).astype(BF16)
        p = p.reshape(w, NL, -1)
        p = jnp.stack(gather(p, "col", ZH, nh, zh), axis=1)
        p = jnp.stack(gather(p, "col", 1, nx, x), axis=3)
        p = p.reshape(w, -1)
        second = jnp.dot(p, b_panel, preferred_element_type=F32)
        scaled.append((second / (el[m * w:(m + 1) * w, None] + er[None, :])).astype(BF16))
    scaled = jnp.concatenate(scaled, axis=0)

    sub = rows_own // (ny * NC * R_CHUNKS)
    qa = jnp.concatenate(left, axis=1)
    qa = qa.reshape(nh, NL, nx, ny, NC, R_CHUNKS, sub, width)
    qa = qa.transpose(5, 4, 3, 1, 2, 0, 6, 7).reshape(R_CHUNKS, -1, width)
    rows = qa.shape[1]

    def add_hops(total, parts, axis, unit):
        for s in range(1, len(parts) + 1):
            total = total + hop(parts[s - 1].astype(BF16), axis, unit * s).astype(F32)
        return total

    def scatter(v, axis, unit, g, me):
        n = v.shape[0] // g
        return add_hops(part(v, me, n), [part(v, me ^ s, n) for s in range(1, g)], axis, unit)

    outs = []
    for q in range(R_CHUNKS):
        half_rows = rows // NC
        give = jnp.dot(part(qa[q], c ^ 1, half_rows), scaled, preferred_element_type=F32)
        keep = jnp.dot(part(qa[q], c, half_rows), scaled, preferred_element_type=F32)
        h = add_hops(keep, [give], "row", 1)
        h = scatter(h, "row", NC, ny, y)
        h = scatter(h, "col", ZL, NL, zl).astype(BF16)
        n = h.shape[0] // nx

        def term(i):
            return lax.dot_general(part(h, i, n), b_panel, (((1,), (1,)), ((), ())), preferred_element_type=F32)

        give = [term(x ^ s) for s in range(1, nx)]
        t = add_hops(term(x), give, "col", 1)
        t = scatter(t, "col", ZH, nh, zh).astype(BF16)
        t = t.reshape(sub, ny * NC, -1)
        got = [lax.dynamic_index_in_dim(t, row, 1, keepdims=False)]
        for s in range(1, ny * NC):
            got.append(hop(lax.dynamic_index_in_dim(t, row ^ s, 1, keepdims=False), "row", s))
        outs.append(jnp.stack(ordered(got, row)))
    return jnp.stack(outs, axis=1).reshape(rows_own, cols_own)


MESH = pl.DeviceIdType.MESH
HT = 512
W = 256
PIECES = 3
NR = 6
VMEM_LIMIT = 67043328


def place():
    col, row = lax.axis_index("col"), lax.axis_index("row")
    x, z = col % 2, col // 2
    return row // 2, row % 2, z // 2, z % 2, x


def device(y, c, zh, zl, x):
    return (y * 2 + c, (zh * 2 + zl) * 2 + x)


def enter(partners):
    barrier = pltpu.get_barrier_semaphore()
    for d in partners:
        pl.semaphore_signal(barrier, inc=1, device_id=d, device_id_type=MESH)
    pl.semaphore_wait(barrier, len(partners))


def first_kernel(rhs, ql, qr, el, er, s_out, qa_out, b_out,
                 cp, bp, qa, qat, pbuf, s, erb, send, recv, local):
    y, c, zh, zl, x = place()
    ry, rc = device(1 - y, c, zh, zl, x), device(y, 1 - c, zh, zl, x)
    rl, rh, rx = device(y, c, zh, 1 - zl, x), device(y, c, 1 - zh, zl, x), device(y, c, zh, zl, 1 - x)
    enter([ry, rc, rl, rh, rx])
    r0, c0 = rhs.shape
    chunks = c0 // W
    rp = r0 // PIECES
    ids = {}

    def push(key, src, dst, dev, when=None):
        k = ids.setdefault(key, len(ids))
        d = pltpu.make_async_remote_copy(src_ref=src, dst_ref=dst, send_sem=send.at[k], recv_sem=recv.at[k],
                                         device_id=dev, device_id_type=MESH)
        started[key] = d
        if when is None:
            d.start()
        else:
            pl.when(when)(d.start)

    started = {}

    def got(key):
        started[key].wait_recv()

    def lanes(i):
        return pl.ds(pl.multiple_of(i, 128), W)

    def qa_at(m, a, b, d):
        return qa.at[m, a, b, d]

    def rows(yy, cc, p):
        return pl.ds(pl.multiple_of((yy * 2 + cc) * r0 + p * rp, 16), rp)

    own = [pltpu.make_async_copy(ql.at[:, :, :, lanes(zl * c0 + m * W)], qa_at(m, zh, zl, x), local.at[m]) for m in range(chunks)]
    own_c = pltpu.make_async_copy(rhs, cp.at[zl, pl.ds(pl.multiple_of((y * 2 + c) * r0, 16), r0)], local.at[chunks])
    own_b = pltpu.make_async_copy(qr, bp.at[zl, pl.ds(pl.multiple_of((y * 2 + c) * r0, 16), r0)], local.at[chunks + 1])
    own_e = pltpu.make_async_copy(er, erb.at[zl], local.at[chunks + 2])
    for d in own + [own_c, own_b, own_e]:
        d.start()

    def panel_push(t, ref, hopname, zz, yy, cc, p, dev, when=None):
        v = ref.at[zz, rows(yy, cc, p)]
        push((t, hopname, p), v, v, dev, when)

    def qa_own(m):
        push(("a", "l", m), ql.at[:, :, :, lanes((1 - zl) * c0 + m * W)], qa_at(m, zh, zl, x), rl)
        push(("a", "h0", m), qa_at(m, zh, zl, x), qa_at(m, zh, zl, x), rh)
        push(("a", "x00", m), qa_at(m, zh, zl, x), qa_at(m, zh, zl, x), rx)

    def qa_l(m):
        got(("a", "l", m))
        v = qa_at(m, zh, 1 - zl, x)
        push(("a", "h1", m), v, v, rh)
        push(("a", "x01", m), v, v, rx)

    def qa_h0(m):
        got(("a", "h0", m))
        v = qa_at(m, 1 - zh, zl, x)
        push(("a", "x10", m), v, v, rx)

    def qa_h1(m):
        got(("a", "h1", m))
        v = qa_at(m, 1 - zh, 1 - zl, x)
        push(("a", "x11", m), v, v, rx)

    def panel_l(t, ref, p):
        got((t, "l", p))
        panel_push(t, ref, "y1", 1 - zl, y, c, p, ry)
        panel_push(t, ref, "c10", 1 - zl, y, c, p, rc)

    def panel_y0(t, ref, p):
        got((t, "y0", p))
        panel_push(t, ref, "c01", zl, 1 - y, c, p, rc)

    def panel_y1(t, ref, p):
        got((t, "y1", p))
        panel_push(t, ref, "c11", 1 - zl, 1 - y, c, p, rc)

    for d in own:
        d.wait()
    own_c.wait()
    qa_own(0)
    for p in range(PIECES):
        panel_push("c", cp, "l", zl, y, c, p, rl)
        panel_push("c", cp, "y0", zl, y, c, p, ry)
        panel_push("c", cp, "c00", zl, y, c, p, rc)
        if p + 1 < chunks:
            qa_own(p + 1)
    for m in range(PIECES + 1, chunks):
        qa_own(m)
    own_e.wait()
    push(("e",), erb.at[zl], erb.at[zl], rl)
    own_b.wait()
    for p in range(PIECES):
        panel_push("b", bp, "c00", zl, y, c, p, rc)

    for m in range(chunks):
        qa_l(m)
        if m < PIECES:
            panel_l("c", cp, m)
        qa_h0(m)
        if m < PIECES:
            panel_y0("c", cp, m)
        if m >= 1:
            qa_h1(m - 1)
            if m - 1 < PIECES:
                panel_y1("c", cp, m - 1)
    for p in range(PIECES):
        panel_push("b", bp, "l", zl, y, c, p, rl, c == 0)
        panel_push("b", bp, "y0", zl, y, c, p, ry)
    qa_h1(chunks - 1)
    for p in range(chunks, PIECES):
        panel_l("c", cp, p)
        panel_y0("c", cp, p)
    for p in range(chunks - 1, PIECES):
        panel_y1("c", cp, p)
    for h in ("c00", "c10", "c01", "c11"):
        for p in range(PIECES):
            got(("c", h, p))

    tiles = 2 * c0 // W
    per = c0 // W

    def project(m):
        for h in ("x00", "x01", "x10", "x11"):
            got(("a", h, m))
        for a in range(2):
            for b in range(2):
                for d in range(2):
                    k = ((a * 2 + b) * 2 + d) * c0
                    qat[:, k:k + c0] = qa[m, a, b, d].reshape(c0, W).T

        @pl.loop(0, tiles)
        def _(nt):
            acc = jnp.dot(qat[...], cp[nt // per, :, pl.ds(pl.multiple_of(nt % per * W, W), W)], preferred_element_type=F32)
            pbuf[m, zh, x, :, pl.ds(pl.multiple_of(nt * W, W), W)] = acc.astype(BF16)

        v = pbuf.at[m, zh, x]
        push(("p", "h", m), v, v, rh)
        push(("p", "x0", m), v, v, rx)

    def forward(m):
        got(("p", "h", m))
        v = pbuf.at[m, 1 - zh, x]
        push(("p", "x1", m), v, v, rx)

    def second(m):
        got(("p", "x0", m))
        got(("p", "x1", m))

        @pl.loop(0, tiles)
        def _(nt):
            acc = None
            for a in range(2):
                for d in range(2):
                    for b in range(2):
                        k = ((a * 2 + b) * 2 + d) * c0
                        t = jnp.dot(pbuf[m, a, d, :, b * c0:(b + 1) * c0],
                                    bp[nt // per, k:k + c0, pl.ds(pl.multiple_of(nt % per * W, W), W)],
                                    preferred_element_type=F32)
                        acc = t if acc is None else acc + t
            den = el[m * W:(m + 1) * W, :] + erb[nt // per, :, pl.ds(pl.multiple_of(nt % per * W, W), W)]
            s[m * W:(m + 1) * W, pl.ds(pl.multiple_of(nt * W, W), W)] = (acc / den).astype(BF16)

    for m in range(chunks):
        project(m)
        if m == 0:
            for p in range(PIECES):
                panel_push("b", bp, "l", zl, y, c, p, rl, c == 1)
        if m < PIECES:
            panel_l("b", bp, m)
            panel_y0("b", bp, m)
    for p in range(chunks, PIECES):
        panel_l("b", bp, p)
        panel_y0("b", bp, p)
    qa_copy = pltpu.make_async_copy(qa, qa_out, local.at[0])
    qa_copy.start()
    for m in range(chunks):
        forward(m)
        if m < PIECES:
            panel_y1("b", bp, m)
    for p in range(chunks, PIECES):
        panel_y1("b", bp, p)
    for h in ("c00", "c10", "c01", "c11"):
        for p in range(PIECES):
            got(("b", h, p))
    b_copy = pltpu.make_async_copy(bp, b_out, local.at[1])
    b_copy.start()
    got(("e",))
    for m in range(chunks):
        second(m)
    s_copy = pltpu.make_async_copy(s, s_out, local.at[2])
    s_copy.start()
    for d in started.values():
        d.wait_send()
    qa_copy.wait()
    b_copy.wait()
    s_copy.wait()


def second_kernel(qa_in, s_in, b_in, out, qa, s, b, recvc, recvy, recvl, givec, givey, givel, hf,
                  recvx, recvh, givex, giveh, fin, keepx, keep, send, recv, outs, outr, local):
    y, c, zh, zl, x = place()
    ry, rc = device(1 - y, c, zh, zl, x), device(y, 1 - c, zh, zl, x)
    rl, rh, rx = device(y, c, zh, 1 - zl, x), device(y, c, 1 - zh, zl, x), device(y, c, zh, zl, 1 - x)
    rd = device(1 - y, 1 - c, zh, zl, x)
    loads = [pltpu.make_async_copy(u, v, local.at[i]) for i, (u, v) in enumerate(((s_in, s), (qa_in, qa), (b_in, b)))]
    for d in loads:
        d.start()
    enter([ry, rc, rl, rh, rx, rd])
    chunks, c0 = qa.shape[0], b.shape[2]
    tiles = 2 * c0 // HT
    quarter = out.shape[-1]
    T = 512
    per = quarter // T

    def hop_of(k, q, src, dst, dev):
        return pltpu.make_async_remote_copy(src_ref=src, dst_ref=dst, send_sem=send.at[k, q], recv_sem=recv.at[k, q],
                                            device_id=dev, device_id_type=MESH)

    def c_hop(q):
        return hop_of(0, q, givec, recvc.at[q], rc)

    def y_hop(q):
        return hop_of(1, q, givey.at[q % 2], recvy.at[q], ry)

    def l_hop(q):
        return hop_of(2, q, givel.at[q % 2], recvl.at[q], rl)

    def x_hop(q):
        return hop_of(3, q, givex.at[q % 2], recvx.at[q], rx)

    def h_hop(q):
        return hop_of(4, q, giveh.at[q % 2], recvh.at[q], rh)

    def out_hops(q):
        yc = y * 2 + c
        hops = []
        for i, (dev, to) in enumerate(((rc, y * 2 + 1 - c), (ry, (1 - y) * 2 + c), (rd, (1 - y) * 2 + 1 - c))):
            hops.append(pltpu.make_async_remote_copy(
                src_ref=fin.at[q % 2, to], dst_ref=out.at[yc, q], send_sem=outs.at[i, q], recv_sem=outr.at[i, q],
                device_id=dev, device_id_type=MESH))
        return hops

    def own_out(q):
        yc = y * 2 + c
        return pltpu.make_async_copy(fin.at[q % 2, yc], out.at[yc, q], local.at[3 + q % 2])

    def cols(nt, n):
        return pl.ds(pl.multiple_of(nt * n, n), n)

    def left_dot(load, nt):
        a = jnp.concatenate([load(m).reshape(-1, W) for m in range(chunks)], axis=1)
        return jnp.dot(a, s[:, cols(nt, HT)], preferred_element_type=F32)

    def wide(v):
        return v.reshape(-1, v.shape[-1]).astype(F32)

    def stage_c(q):
        @pl.when(q >= 1)
        def _():
            c_hop(q - 1).wait_send()

        @pl.loop(0, 2 * tiles)
        def _(t):
            yy, nt = t // tiles, t % tiles
            acc = left_dot(lambda m: qa[m, :, :, :, yy * 2 + 1 - c, q], nt)
            givec[yy, :, :, :, :, cols(nt, HT)] = acc.astype(BF16).reshape(givec.shape[1:5] + (HT,))

        c_hop(q).start()

    def stage_y(q):
        c_hop(q).wait_recv()

        @pl.when(q >= 2)
        def _():
            y_hop(q - 2).wait_send()

        @pl.loop(0, tiles)
        def _(nt):
            acc = left_dot(lambda m: qa[m, :, :, :, (1 - y) * 2 + c, q], nt)
            acc = acc + wide(recvc[q, 1 - y, :, :, :, :, cols(nt, HT)])
            givey[q % 2, :, :, :, :, cols(nt, HT)] = acc.astype(BF16).reshape(givey.shape[1:5] + (HT,))

        y_hop(q).start()

    def stage_l(q):
        y_hop(q).wait_recv()

        @pl.when(q >= 2)
        def _():
            l_hop(q - 2).wait_send()

        @pl.loop(0, tiles)
        def _(nt):
            acc = left_dot(lambda m: qa[m, :, 1 - zl, :, y * 2 + c, q], nt)
            acc = acc + wide(recvc[q, y, :, 1 - zl, :, :, cols(nt, HT)]) + wide(recvy[q, :, 1 - zl, :, :, cols(nt, HT)])
            givel[q % 2, :, :, :, cols(nt, HT)] = acc.astype(BF16).reshape(givel.shape[1:4] + (HT,))

        l_hop(q).start()

    def right_dot(h, ct):
        acc = None
        for k in range(2):
            t = lax.dot_general(h[:, k * c0:(k + 1) * c0], b[k, cols(ct, T), :], (((1,), (1,)), ((), ())), preferred_element_type=F32)
            acc = t if acc is None else acc + t
        return acc

    def stage_x(q):
        l_hop(q).wait_recv()

        @pl.loop(0, tiles)
        def _(nt):
            acc = left_dot(lambda m: qa[m, :, zl, :, y * 2 + c, q], nt)
            acc = acc + wide(recvc[q, y, :, zl, :, :, cols(nt, HT)]) + wide(recvy[q, :, zl, :, :, cols(nt, HT)])
            acc = acc + wide(recvl[q, :, :, :, cols(nt, HT)])
            v = acc.astype(BF16).reshape(2, 2, -1, HT)
            for d in range(2):
                hf[d, :, :, cols(nt, HT)] = v[:, d]

        @pl.when(q >= 2)
        def _():
            x_hop(q - 2).wait_send()

        @pl.when(q == 0)
        def _():
            loads[2].wait()

        @pl.loop(0, 4 * per)
        def _(ct):
            v = right_dot(hf[...].reshape(-1, 2 * c0), ct).reshape(2, 2, -1, T)
            low = x == 0
            at = (slice(None), ct // per, slice(None), cols(ct % per, T))
            givex[(q % 2,) + at] = jnp.where(low, v[1], v[0]).astype(BF16)
            keepx[(q % 2,) + at] = jnp.where(low, v[0], v[1])

        x_hop(q).start()

    def stage_h(q):
        x_hop(q).wait_recv()

        @pl.when(q >= 2)
        def _():
            h_hop(q - 2).wait_send()

        @pl.loop(0, 4 * per)
        def _(ct):
            i, k = ct // per, cols(ct % per, T)
            giveh[q % 2, i, :, k] = (keepx[q % 2, 1 - zh, i, :, k] + recvx[q, 1 - zh, i, :, k].astype(F32)).astype(BF16)
            keep[q % 2, i, :, k] = keepx[q % 2, zh, i, :, k] + recvx[q, zh, i, :, k].astype(F32)

        h_hop(q).start()

    def stage_o(q):
        h_hop(q).wait_recv()

        @pl.when(q >= 2)
        def _():
            for d in out_hops(q - 2):
                d.wait_send()
            own_out(q - 2).wait()

        @pl.loop(0, 4)
        def _(i):
            fin[q % 2, i] = (keep[q % 2, i] + recvh[q, i].astype(F32)).astype(BF16)

        for d in out_hops(q):
            d.start()
        own_out(q).start()

    loads[0].wait()
    loads[1].wait()
    stages = (stage_c, stage_y, stage_l, stage_x, stage_h, stage_o)

    @pl.loop(0, NR + len(stages) - 1)
    def _(t):
        for lag, stage in enumerate(stages):
            @pl.when((t >= lag) & (t < lag + NR))
            def _(stage=stage, lag=lag):
                stage(t - lag)

    c_hop(NR - 1).wait_send()
    for q in (NR - 2, NR - 1):
        y_hop(q).wait_send()
        l_hop(q).wait_send()
        x_hop(q).wait_send()
        h_hop(q).wait_send()
        for d in out_hops(q):
            d.wait_send()
        own_out(q).wait()
    for q in range(NR):
        for d in out_hops(q):
            d.wait_recv()


def kernels(rhs, basis_left, basis_right, eig_left, eig_right):
    r0, c0 = rhs.shape
    n = 4 * r0
    chunks = c0 // W
    sub = c0 // (4 * NR)
    zl = lax.rem(lax.div(lax.axis_index("col"), 2), 2)
    el = lax.dynamic_slice_in_dim(eig_left, zl * c0, c0, axis=0)[:, None]
    any_spec = pl.BlockSpec(memory_space=pl.ANY)
    vmem = pl.BlockSpec(memory_space=pltpu.VMEM)
    qa_shape = (chunks, 2, 2, 2, 4, NR, sub, W)
    copies = 2 * 7 * PIECES + 10 * chunks + 1
    dma = pltpu.SemaphoreType.DMA
    s, qa, b = pl.pallas_call(
        first_kernel,
        out_shape=(jax.ShapeDtypeStruct((c0, 2 * c0), BF16), jax.ShapeDtypeStruct(qa_shape, BF16),
                   jax.ShapeDtypeStruct((2, n, c0), BF16)),
        in_specs=[any_spec, any_spec, any_spec, vmem, any_spec],
        out_specs=(any_spec, any_spec, any_spec),
        scratch_shapes=[
            pltpu.VMEM((2, n, c0), BF16), pltpu.VMEM((2, n, c0), BF16), pltpu.VMEM(qa_shape, BF16),
            pltpu.VMEM((W, n), BF16), pltpu.VMEM((chunks, 2, 2, W, 2 * c0), BF16), pltpu.VMEM((c0, 2 * c0), BF16),
            pltpu.VMEM((2, 1, c0), F32), dma((copies,)), dma((copies,)), dma((chunks + 3,))],
        compiler_params=pltpu.CompilerParams(collective_id=0, has_side_effects=True, vmem_limit_bytes=VMEM_LIMIT),
        name="first_half",
    )(rhs, basis_left.reshape(4, NR, sub, 2 * c0), basis_right, el, eig_right[None, :])
    out = pl.pallas_call(
        second_kernel,
        out_shape=jax.ShapeDtypeStruct((4, NR, sub, r0), BF16),
        in_specs=[any_spec] * 3,
        out_specs=any_spec,
        scratch_shapes=[
            pltpu.VMEM(qa_shape, BF16), pltpu.VMEM((c0, 2 * c0), BF16), pltpu.VMEM((2, n, c0), BF16),
            pltpu.VMEM((NR, 2, 2, 2, 2, sub, 2 * c0), BF16), pltpu.VMEM((NR, 2, 2, 2, sub, 2 * c0), BF16),
            pltpu.VMEM((NR, 2, 2, sub, 2 * c0), BF16),
            pltpu.VMEM((2, 2, 2, 2, sub, 2 * c0), BF16), pltpu.VMEM((2, 2, 2, 2, sub, 2 * c0), BF16),
            pltpu.VMEM((2, 2, 2, sub, 2 * c0), BF16), pltpu.VMEM((2, 2, sub, 2 * c0), BF16),
            pltpu.VMEM((NR, 2, 4, sub, r0), BF16), pltpu.VMEM((NR, 4, sub, r0), BF16),
            pltpu.VMEM((2, 2, 4, sub, r0), BF16), pltpu.VMEM((2, 4, sub, r0), BF16),
            pltpu.VMEM((2, 4, sub, r0), BF16), pltpu.VMEM((2, 2, 4, sub, r0), F32), pltpu.VMEM((2, 4, sub, r0), F32),
            dma((5, NR)), dma((5, NR)), dma((3, NR)), dma((3, NR)), dma((5,))],
        compiler_params=pltpu.CompilerParams(collective_id=1, has_side_effects=True, vmem_limit_bytes=VMEM_LIMIT),
        name="second_half",
    )(qa, s, b)
    return out.reshape(c0, r0)


def fits(nz, nx, ny, rows, cols):
    return nz == 4 and nx == 2 and ny == 2 and rows == 2 * cols and cols % (4 * NR * 16) == 0 and cols % W == 0 and rows % 512 == 0


def step(nz, nx, *arrays):
    rows, cols = arrays[0].shape
    if fits(nz, nx, lax.axis_size("row") // NC, rows, cols):
        return kernels(*arrays)
    return body(nz, nx, *arrays)


def solution(mesh):
    nz = mesh.shape["row"]
    nx = mesh.shape["col"] // nz
    in_specs = (P("row", "col"), P("col", "row"), P("row", "col"), P("row"), P("col"))
    fn = functools.partial(step, nz, nx)
    return jax.shard_map(fn, mesh=mesh, in_specs=in_specs, out_specs=P("col", "row"), check_vma=False)
```
